32 devices in a mesh: leaf: 32 (over z, y, x, core).
Axes of the slice: x: 2, y: 2, z: 4, core: 2. Of those that a mesh axis runs over, the one named last changes fastest.
Arguments:
- random_block: bfloat16 [16384, 256], P('leaf'), may hold values from -6 to 6
- diag_block: bfloat16 [16384, 512], P('leaf'), may hold values from -0.25 to 0.25
- basis_out: bfloat16 [16384, 256], P('leaf'), may hold values from -0.1875 to 0.1875
- basis_in: bfloat16 [16384, 256], P('leaf'), may hold values from -0.25 to 0.25
- low_up: bfloat16 [32, 2, 256, 256], P('leaf'), as said below
- low_down: bfloat16 [32, 2, 256, 256], P('leaf'), as said below
- low_coupling: bfloat16 [32, 2, 256, 256], P('leaf'), as said below
- top_up: bfloat16 [12, 256, 256], replicated, may hold values from -0.25 to 0.25
- top_down: bfloat16 [12, 256, 256], replicated, may hold values from -0.375 to 0.375
- top_coupling: bfloat16 [14, 256, 256], replicated, may hold values from -0.375 to 0.375
Outputs:
- sample: bfloat16 [16384, 256], P('leaf')
The draws below stay inside these ranges and needn't reach their ends.
Inputs may be any that keep to these rules, and one draw needn't show every extreme that they name: `low_up`: for every level l below 2, entries [i, l] and [j, l] are the same matrix when i // 2^l == j // 2^l. `low_down`: for every level l below 2, entries [i, l] and [j, l] are the same matrix when i // 2^l == j // 2^l. `low_coupling`: for every level l below 2, entries [i, l] and [j, l] are the same matrix when i // 2^l == j // 2^l.
All inputs are finite; a program needn't handle non-finite values.
Results may differ from the reference program's by a relative error of at most 0.018.
Values may be sent and summed in bfloat16 or wider, within the bound.
A program may use at most 64 MiB of HBM per device.

```python
import jax
import jax.numpy as jnp

LEAF = 512
RANK = 256
NCOL = 256
TOP = 3
LOW = 2
ORDER = 16384
TOPNODES = 14
TOPINNER = 12
N_LEAF = 32


def replicated_levels(key, scale):
    leaves = ORDER // LEAF
    stacked = []
    for height in range(LOW):
        node_count = leaves // 2 ** height
        subkey = jax.random.fold_in(key, height)
        values = jax.random.normal(subkey, (node_count, RANK, RANK), jnp.float32) * scale
        stacked.append(jnp.repeat(values, 2 ** height, axis=0))
    return jnp.stack(stacked, axis=1).astype(jnp.bfloat16)


def draw_low_up(key, part):
    return replicated_levels(jax.random.fold_in(key, 101), (2.0 * RANK) ** (-0.5))


def draw_low_down(key, part):
    return replicated_levels(jax.random.fold_in(key, 202), RANK ** (-0.5))


def draw_low_coupling(key, part):
    return replicated_levels(jax.random.fold_in(key, 303), RANK ** (-0.5))


def levels(stream_key, shape, shards, low, top_value):
    def one(position, blocks):
        draws = jax.random.uniform(jax.random.fold_in(jax.random.fold_in(stream_key, 6), position), (blocks,), jnp.float32, low / len(shards), top_value / len(shards))
        return jnp.repeat(jnp.exp(draws), shape[position] // blocks).reshape((-1,) + (1,) * (len(shape) - position - 1))

    level = one(*shards[0])
    for cut in shards[1:]:
        level = level * one(*cut)
    return level


def normal_values(stream_key, dims, scale, reach, pieces=(), kind=jnp.bfloat16):
    drawn = jax.random.normal(stream_key, dims, jnp.float32) * scale
    if len(pieces) > 0:
        drawn = levels(stream_key, dims, pieces, -0.22, 0.18) * drawn
    return jnp.clip(drawn, min=-reach, max=reach).astype(kind)


def setup_inputs(seed: int = 0) -> dict:
    streams_of = jax.random.split(jax.random.key(seed), 11)
    random_block = normal_values(streams_of[0], (ORDER, NCOL), 1.0, 6.0, ((0, 32),))
    diag_block = normal_values(streams_of[1], (ORDER, LEAF), LEAF ** -0.5, 0.25, ((0, 32),))
    basis_out = normal_values(streams_of[2], (ORDER, RANK), (4 * RANK) ** -0.5, 0.1875, ((0, 32),))
    basis_in = normal_values(streams_of[3], (ORDER, RANK), LEAF ** -0.5, 0.25, ((0, 32),))
    low_up = draw_low_up(jax.random.fold_in(streams_of[10], 71), 0)
    low_down = draw_low_down(jax.random.fold_in(streams_of[10], 71), 0)
    low_coupling = draw_low_coupling(jax.random.fold_in(streams_of[10], 71), 0)
    top_up = normal_values(streams_of[7], (TOPINNER, RANK, RANK), (2 * RANK) ** -0.5, 0.25)
    top_down = normal_values(streams_of[8], (TOPINNER, RANK, RANK), RANK ** -0.5, 0.375)
    top_coupling = normal_values(streams_of[9], (TOPNODES, RANK, RANK), RANK ** -0.5, 0.375)
    return {"random_block": random_block, "diag_block": diag_block, "basis_out": basis_out, "basis_in": basis_in, "low_up": low_up, "low_down": low_down, "low_coupling": low_coupling, "top_up": top_up, "top_down": top_down, "top_coupling": top_coupling}


def level_generators(lower, upper, height, low_levels):
    if height < low_levels:
        return lower[:: 2 ** height, height]
    section = height - low_levels
    offset = 2 ** (TOP + 1) - 2 ** (TOP + 1 - section)
    node_count = 2 ** (TOP - section)
    return upper[offset:offset + node_count]


def batch_trans(matrix, values):
    return jnp.einsum("nrs,nrc->nsc", matrix.astype(jnp.float32), values.astype(jnp.float32))


def batch_apply(matrix, values):
    return jnp.einsum("nrs,nsc->nrc", matrix.astype(jnp.float32), values.astype(jnp.float32))


def reference(random_block, diag_block, basis_out, basis_in, low_up, low_down, low_coupling, top_up, top_down, top_coupling):
    levels_total = N_LEAF.bit_length() - 1
    low_levels = levels_total - TOP
    leaf_cols = random_block.reshape(N_LEAF, LEAF, NCOL)
    current = batch_trans(basis_in.reshape(N_LEAF, LEAF, RANK), leaf_cols)
    couplings = []
    for height in range(levels_total):
        node_count = current.shape[0]
        rounded = current.astype(jnp.bfloat16)
        swapped = rounded.reshape(node_count // 2, 2, RANK, NCOL)[:, ::-1].reshape(node_count, RANK, NCOL)
        coupler = level_generators(low_coupling, top_coupling, height, low_levels)
        couplings.append(batch_apply(coupler, swapped))
        if height < levels_total - 1:
            lifter = level_generators(low_up, top_up, height, low_levels)
            lifted = batch_trans(lifter, rounded).astype(jnp.bfloat16).astype(jnp.float32)
            paired = lifted.reshape(node_count // 2, 2, RANK, NCOL)
            current = paired[:, 0] + paired[:, 1]
    descent = couplings[-1]
    for height in range(levels_total - 2, -1, -1):
        parent = jnp.repeat(descent.astype(jnp.bfloat16), 2, axis=0)
        lowering = level_generators(low_down, top_down, height, low_levels)
        descent = batch_apply(lowering, parent) + couplings[height]
    local = batch_apply(diag_block.reshape(N_LEAF, LEAF, LEAF), leaf_cols)
    spread = batch_apply(basis_out.reshape(N_LEAF, LEAF, RANK), descent.astype(jnp.bfloat16))
    return (local + spread).reshape(ORDER, NCOL).astype(jnp.bfloat16)
```

```python
import functools

import jax
import jax.numpy as jnp
from jax import lax
from jax.experimental import pallas as pl
from jax.experimental.pallas import tpu as pltpu
from jax.sharding import PartitionSpec as P

TOP = 3
CHUNKS = 2
MESH = pl.DeviceIdType.MESH


def nn(a, b):
    return jnp.dot(a, b, preferred_element_type=jnp.float32)


def nt(a, b):
    return lax.dot_general(a, b, (((1,), (1,)), ((), ())), preferred_element_type=jnp.float32)


def tn(a, b):
    return lax.dot_general(a, b, (((0,), (0,)), ((), ())), preferred_element_type=jnp.float32)


def bf(a):
    return a.astype(jnp.bfloat16)


def f32(a):
    return a.astype(jnp.float32)


def kernel(levels, low, x, d, u, v, lup, ldn, lcp, tup, tdn, tcp, out,
           xs, dv, uv, vv, wv, wsib, rv, bv, cb0, rcb0, scb, rcb, slift, rlift, own, fl, f0, acc,
           zb1, rz1, in_sem, s0, r0, scs, rcs, sls, rls, szs, rzs):
    me = lax.axis_index("leaf")
    side = lax.rem(me, 2)
    half = xs.shape[2]
    step = half // CHUNKS

    def bit_partner(height):
        stride = 2 ** height
        bit = lax.rem(me // stride, 2)
        return me + stride - 2 * stride * bit

    partners = [bit_partner(height) for height in range(levels)]

    loads = []

    def load(src, dst):
        copy = pltpu.make_async_copy(src, dst, in_sem.at[len(loads)])
        copy.start()
        loads.append(copy)
        return copy

    def node(height):
        section = height - low
        return 2 ** (TOP + 1) - 2 ** (TOP + 1 - section) + me // 2 ** height

    def node_sib(height):
        section = height - low
        return 2 ** (TOP + 1) - 2 ** (TOP + 1 - section) + partners[height] // 2 ** height

    other_cols = pl.ds(pl.multiple_of((1 - side) * half, half), half)
    self_cols = pl.ds(pl.multiple_of(side * half, half), half)
    ld_v = load(v, vv)
    ld_xo = load(x.at[:, other_cols], xs.at[0])
    ld_w, ld_ws, ld_r, ld_b = {}, {}, {}, {}
    ld_w[0] = load(lup.at[0, 0], wv.at[0])
    ld_xs = load(x.at[:, self_cols], xs.at[1])

    barrier = pltpu.get_barrier_semaphore()
    for partner in partners:
        pl.semaphore_signal(barrier, inc=1, device_id=(partner,), device_id_type=MESH)

    for height in range(1, levels - 1):
        if height < low:
            ld_w[height] = load(lup.at[0, height], wv.at[height])
        else:
            ld_w[height] = load(tup.at[node(height)], wv.at[height])
            ld_ws[height] = load(tup.at[node_sib(height)], wsib.at[height - low])
    ld_d = load(d, dv)
    for height in range(levels):
        ld_b[height] = load(lcp.at[0, height] if height < low else tcp.at[node(height)], bv.at[height])
    for height in range(levels - 2, -1, -1):
        ld_r[height] = load(ldn.at[0, height] if height < low else tdn.at[node(height)], rv.at[height])
    ld_u = load(u, uv)

    sent = []

    def send(src, dst, ssem, rsem, partner):
        copy = pltpu.make_async_remote_copy(
            src_ref=src, dst_ref=dst, send_sem=ssem, recv_sem=rsem,
            device_id=(partner,), device_id_type=MESH,
        )
        copy.start()
        sent.append(copy)
        return copy

    ld_v.wait()
    ld_xo.wait()
    cb0[0] = bf(tn(xs[0], vv[...]))
    ld_w[0].wait()
    slift[0] = bf(nn(cb0[0], wv[0]))
    pl.semaphore_wait(barrier, levels)
    rl = {}
    rc = {}
    for k in range(CHUNKS):
        rows = pl.ds(k * step, step)
        rl[0, k] = send(slift.at[0, rows], rlift.at[0, rows], sls.at[0, k], rls.at[0, k], partners[0])
    ld_xs.wait()
    cb0[1] = bf(tn(xs[1], vv[...]))
    own[0] = bf(nn(cb0[1], wv[0]))
    rc0 = [send(cb0.at[j], rcb0.at[1 - j], s0.at[j], r0.at[j], partners[0]) for j in range(2)]

    for height in range(1, levels):
        if height < levels - 1:
            ld_w[height].wait()
        if height > low:
            ld_ws[height - 1].wait()
        for k in range(CHUNKS):
            rows = pl.ds(k * step, step)
            if height <= low:
                rl[height - 1, k].wait_recv()
                theirs = rlift[height - 1, rows]
            else:
                rc[height - 1, k].wait_recv()
                theirs = bf(nn(rcb[height - 1, rows], wsib[height - 1 - low]))
            c = f32(own[height - 1, rows]) + f32(theirs)
            scb[height, rows] = bf(c)
            if height < low:
                lifted = bf(nn(bf(c), wv[height]))
                slift[height, rows] = lifted
                own[height, rows] = lifted
                rl[height, k] = send(slift.at[height, rows], rlift.at[height, rows],
                                     sls.at[height, k], rls.at[height, k], partners[height])
            else:
                rc[height, k] = send(scb.at[height, rows], rcb.at[height, rows],
                                     scs.at[height, k], rcs.at[height, k], partners[height])
        if height < low:
            for k in range(CHUNKS):
                rows = pl.ds(k * step, step)
                rc[height, k] = send(scb.at[height, rows], rcb.at[height, rows],
                                     scs.at[height, k], rcs.at[height, k], partners[height])
        elif height < levels - 1:
            own[height] = bf(nn(scb[height], wv[height]))
        if height == 1:
            ld_d.wait()
            for j in range(2):
                acc[j] = nn(dv[...], xs[j])
        if height == 2:
            ld_b[0].wait()
            for j in range(2):
                rc0[1 - j].wait_recv()
                f0[j] = nt(rcb0[j], bv[0])
        if height > low:
            ld_b[height - 1].wait()
            fl[height - 1] = nt(rcb[height - 1], bv[height - 1])
        if height == levels - 1:
            for lower in range(1, low):
                ld_b[lower].wait()
                for k in range(CHUNKS):
                    rc[lower, k].wait_recv()
                fl[lower] = nt(rcb[lower], bv[lower])

    ld_b[levels - 1].wait()
    for height in range(levels - 2, -1, -1):
        ld_r[height].wait()
    ld_u.wait()
    rz = []
    for k in range(CHUNKS):
        rows = pl.ds(k * step, step)
        rc[levels - 1, k].wait_recv()
        z = nt(rcb[levels - 1, rows], bv[levels - 1])
        for height in range(levels - 2, 0, -1):
            z = nt(bf(z), rv[height]) + fl[height, rows]
        zb1[rows] = bf(z)
        rz.append(send(zb1.at[rows], rz1.at[rows], szs.at[k], rzs.at[k], partners[0]))
    z0 = nt(zb1[...], rv[0]) + f0[1]
    out[:, self_cols] = bf(acc[1] + nt(uv[...], bf(z0)))
    for copy in rz:
        copy.wait_recv()
    z0 = nt(rz1[...], rv[0]) + f0[0]
    out[:, other_cols] = bf(acc[0] + nt(uv[...], bf(z0)))
    for copy in sent:
        copy.wait_send()


def per_device(random_block, diag_block, basis_out, basis_in, low_up, low_down, low_coupling,
               top_up, top_down, top_coupling):
    levels = lax.axis_size("leaf").bit_length() - 1
    low = low_up.shape[1]
    leaf, ncol = random_block.shape
    rank = basis_in.shape[1]
    half = ncol // 2
    b16, f4 = jnp.bfloat16, jnp.float32
    dma = pltpu.SemaphoreType.DMA
    hbm = pl.BlockSpec(memory_space=pltpu.HBM)
    return pl.pallas_call(
        functools.partial(kernel, levels, low),
        out_shape=jax.ShapeDtypeStruct((leaf, ncol), b16),
        in_specs=[hbm] * 10,
        out_specs=pl.BlockSpec(memory_space=pltpu.VMEM),
        scratch_shapes=[
            pltpu.VMEM((2, leaf, half), b16),
            pltpu.VMEM((leaf, leaf), b16),
            pltpu.VMEM((leaf, rank), b16),
            pltpu.VMEM((leaf, rank), b16),
            pltpu.VMEM((levels - 1, rank, rank), b16),
            pltpu.VMEM((TOP - 1, rank, rank), b16),
            pltpu.VMEM((levels - 1, rank, rank), b16),
            pltpu.VMEM((levels, rank, rank), b16),
            pltpu.VMEM((2, half, rank), b16),
            pltpu.VMEM((2, half, rank), b16),
            pltpu.VMEM((levels, half, rank), b16),
            pltpu.VMEM((levels, half, rank), b16),
            pltpu.VMEM((low, half, rank), b16),
            pltpu.VMEM((low, half, rank), b16),
            pltpu.VMEM((levels - 1, half, rank), b16),
            pltpu.VMEM((levels - 1, half, rank), f4),
            pltpu.VMEM((2, half, rank), f4),
            pltpu.VMEM((2, leaf, half), f4),
            pltpu.VMEM((half, rank), b16),
            pltpu.VMEM((half, rank), b16),
            dma((4 * levels + 8,)),
            dma((2,)),
            dma((2,)),
            dma((levels, CHUNKS)),
            dma((levels, CHUNKS)),
            dma((low, CHUNKS)),
            dma((low, CHUNKS)),
            dma((CHUNKS,)),
            dma((CHUNKS,)),
        ],
        compiler_params=pltpu.CompilerParams(collective_id=0, has_side_effects=True),
    )(random_block, diag_block, basis_out, basis_in, low_up, low_down, low_coupling,
      top_up, top_down, top_coupling)


def solution(mesh):
    rows = P("leaf", None)
    gens = P("leaf", None, None, None)
    return jax.shard_map(
        per_device, mesh=mesh,
        in_specs=(rows, rows, rows, rows, gens, gens, gens, P(), P(), P()),
        out_specs=rows, check_vma=False,
    )
```

```python
import functools

import jax
import jax.numpy as jnp
from jax import lax
from jax.experimental import pallas as pl
from jax.experimental.pallas import tpu as pltpu
from jax.sharding import PartitionSpec as P

TOP = 3
CHUNKS = 4
MESH = pl.DeviceIdType.MESH


def nn(a, b):
    return jnp.dot(a, b, preferred_element_type=jnp.float32)


def nt(a, b):
    return lax.dot_general(a, b, (((1,), (1,)), ((), ())), preferred_element_type=jnp.float32)


def tn(a, b):
    return lax.dot_general(a, b, (((0,), (0,)), ((), ())), preferred_element_type=jnp.float32)


def bf(a):
    return a.astype(jnp.bfloat16)


def f32(a):
    return a.astype(jnp.float32)


def kernel(levels, low, x, d, u, v, lup, ldn, lcp, tup, tdn, tcp, out,
           xs, dv, uv, vv, wv, wsib, rv, bv, cb0, rcb0, scb, rcb, slift, rlift, own, fl, f0, acc,
           zb1, rz1, comp, path, zs, in_sem, s0, r0, scs, rcs, sls, rls, szs, rzs):
    me = lax.axis_index("leaf")
    side = lax.rem(me, 2)
    half = xs.shape[2]
    step = half // CHUNKS

    def bit_partner(height):
        stride = 2 ** height
        bit = lax.rem(me // stride, 2)
        return me + stride - 2 * stride * bit

    partners = [bit_partner(height) for height in range(levels)]

    loads = []

    def load(src, dst):
        copy = pltpu.make_async_copy(src, dst, in_sem.at[len(loads)])
        copy.start()
        loads.append(copy)
        return copy

    def node(height):
        section = height - low
        return 2 ** (TOP + 1) - 2 ** (TOP + 1 - section) + me // 2 ** height

    def node_sib(height):
        section = height - low
        return 2 ** (TOP + 1) - 2 ** (TOP + 1 - section) + partners[height] // 2 ** height

    other_cols = pl.ds(pl.multiple_of((1 - side) * half, half), half)
    self_cols = pl.ds(pl.multiple_of(side * half, half), half)
    ld_v = load(v, vv)
    ld_xo = load(x.at[:, other_cols], xs.at[0])
    ld_w, ld_ws, ld_r, ld_b = {}, {}, {}, {}
    ld_w[0] = load(lup.at[0, 0], wv.at[0])
    ld_xs = load(x.at[:, self_cols], xs.at[1])

    barrier = pltpu.get_barrier_semaphore()
    for partner in partners:
        pl.semaphore_signal(barrier, inc=1, device_id=(partner,), device_id_type=MESH)

    for height in range(1, levels - 1):
        if height < low:
            ld_w[height] = load(lup.at[0, height], wv.at[height])
        else:
            ld_w[height] = load(tup.at[node(height)], wv.at[height])
            ld_ws[height] = load(tup.at[node_sib(height)], wsib.at[height - low])
    ld_d = load(d, dv)
    for height in range(levels):
        ld_b[height] = load(lcp.at[0, height] if height < low else tcp.at[node(height)], bv.at[height])
    for height in range(levels - 2, -1, -1):
        ld_r[height] = load(ldn.at[0, height] if height < low else tdn.at[node(height)], rv.at[height])
    ld_u = load(u, uv)

    sent = []

    def send(src, dst, ssem, rsem, partner):
        copy = pltpu.make_async_remote_copy(
            src_ref=src, dst_ref=dst, send_sem=ssem, recv_sem=rsem,
            device_id=(partner,), device_id_type=MESH,
        )
        copy.start()
        sent.append(copy)
        return copy

    ld_v.wait()
    ld_xo.wait()
    cb0[0] = bf(tn(xs[0], vv[...]))
    ld_w[0].wait()
    slift[0] = bf(nn(cb0[0], wv[0]))
    pl.semaphore_wait(barrier, levels)
    rl = {}
    rc = {}
    for k in range(CHUNKS):
        rows = pl.ds(k * step, step)
        rl[0, k] = send(slift.at[0, rows], rlift.at[0, rows], sls.at[0, k], rls.at[0, k], partners[0])
    ld_xs.wait()
    cb0[1] = bf(tn(xs[1], vv[...]))
    own[0] = bf(nn(cb0[1], wv[0]))
    rc0 = [send(cb0.at[j], rcb0.at[1 - j], s0.at[j], r0.at[j], partners[0]) for j in range(2)]

    for height in range(1, levels):
        if height < levels - 1:
            ld_w[height].wait()
        if height > low:
            ld_ws[height - 1].wait()
        for k in range(CHUNKS):
            rows = pl.ds(k * step, step)
            if height <= low:
                rl[height - 1, k].wait_recv()
                theirs = rlift[height - 1, rows]
            else:
                rc[height - 1, k].wait_recv()
                theirs = bf(nn(rcb[height - 1, rows], wsib[height - 1 - low]))
            c = f32(own[height - 1, rows]) + f32(theirs)
            scb[height, rows] = bf(c)
            if height < low:
                lifted = bf(nn(bf(c), wv[height]))
                slift[height, rows] = lifted
                own[height, rows] = lifted
                rl[height, k] = send(slift.at[height, rows], rlift.at[height, rows],
                                     sls.at[height, k], rls.at[height, k], partners[height])
            else:
                rc[height, k] = send(scb.at[height, rows], rcb.at[height, rows],
                                     scs.at[height, k], rcs.at[height, k], partners[height])
        if height < low:
            for k in range(CHUNKS):
                rows = pl.ds(k * step, step)
                rc[height, k] = send(scb.at[height, rows], rcb.at[height, rows],
                                     scs.at[height, k], rcs.at[height, k], partners[height])
        elif height < levels - 1:
            own[height] = bf(nn(scb[height], wv[height]))
        if height == 1:
            ld_d.wait()
            for j in range(2):
                acc[j] = nn(dv[...], xs[j])
        if height == min(2, levels - 1):
            ld_b[0].wait()
            for j in range(2):
                rc0[1 - j].wait_recv()
                f0[j] = nt(rcb0[j], bv[0])
        if height == min(3, levels - 1):
            ld_b[levels - 1].wait()
            for up in range(levels - 2, 0, -1):
                ld_r[up].wait()
                comp[...] = bf(nn(rv[up], bv[levels - 1] if up == levels - 2 else comp[...]))
            ld_r[0].wait()
            ld_u.wait()
            path[...] = bf(nn(uv[...], rv[0]))
            path[...] = bf(nn(path[...], comp[...]))
        if height > low:
            ld_b[height - 1].wait()
            fl[height - 1] = nt(rcb[height - 1], bv[height - 1])
        if height == levels - 1:
            for lower in range(1, low):
                ld_b[lower].wait()
                for k in range(CHUNKS):
                    rc[lower, k].wait_recv()
                fl[lower] = nt(rcb[lower], bv[lower])
            z = fl[levels - 2]
            for up in range(levels - 3, 0, -1):
                z = nt(bf(z), rv[up]) + fl[up]
            zb1[0] = bf(z)
            zsend = send(zb1.at[0], zb1.at[1], zs.at[0], zs.at[1], partners[0])
            z0 = nt(zb1[0], rv[0]) + f0[1]
            acc[1] += nt(uv[...], bf(z0))
            zsend.wait_recv()
            z0 = nt(zb1[1], rv[0]) + f0[0]
            acc[0] += nt(uv[...], bf(z0))

    rz = []
    for k in range(CHUNKS):
        rows = pl.ds(k * step, step)
        rc[levels - 1, k].wait_recv()
        rz.append(send(rcb.at[levels - 1, rows], rz1.at[rows], szs.at[k], rzs.at[k], partners[0]))
    out[:, self_cols] = bf(acc[1] + nt(path[...], rcb[levels - 1]))
    for copy in rz:
        copy.wait_recv()
    out[:, other_cols] = bf(acc[0] + nt(path[...], rz1[...]))
    for copy in sent:
        copy.wait_send()


def per_device(random_block, diag_block, basis_out, basis_in, low_up, low_down, low_coupling,
               top_up, top_down, top_coupling):
    levels = lax.axis_size("leaf").bit_length() - 1
    low = low_up.shape[1]
    leaf, ncol = random_block.shape
    rank = basis_in.shape[1]
    half = ncol // 2
    b16, f4 = jnp.bfloat16, jnp.float32
    dma = pltpu.SemaphoreType.DMA
    hbm = pl.BlockSpec(memory_space=pltpu.HBM)
    return pl.pallas_call(
        functools.partial(kernel, levels, low),
        out_shape=pltpu.VMEM((leaf, ncol), b16),
        in_specs=[hbm] * 10,
        out_specs=pl.BlockSpec(memory_space=pltpu.VMEM),
        scratch_shapes=[
            pltpu.VMEM((2, leaf, half), b16),
            pltpu.VMEM((leaf, leaf), b16),
            pltpu.VMEM((leaf, rank), b16),
            pltpu.VMEM((leaf, rank), b16),
            pltpu.VMEM((levels - 1, rank, rank), b16),
            pltpu.VMEM((TOP - 1, rank, rank), b16),
            pltpu.VMEM((levels - 1, rank, rank), b16),
            pltpu.VMEM((levels, rank, rank), b16),
            pltpu.VMEM((2, half, rank), b16),
            pltpu.VMEM((2, half, rank), b16),
            pltpu.VMEM((levels, half, rank), b16),
            pltpu.VMEM((levels, half, rank), b16),
            pltpu.VMEM((low, half, rank), b16),
            pltpu.VMEM((low, half, rank), b16),
            pltpu.VMEM((levels - 1, half, rank), b16),
            pltpu.VMEM((levels - 1, half, rank), f4),
            pltpu.VMEM((2, half, rank), f4),
            pltpu.VMEM((2, leaf, half), f4),
            pltpu.VMEM((2, half, rank), b16),
            pltpu.VMEM((half, rank), b16),
            pltpu.VMEM((rank, rank), b16),
            pltpu.VMEM((leaf, rank), b16),
            dma((2,)),
            dma((4 * levels + 8,)),
            dma((2,)),
            dma((2,)),
            dma((levels, CHUNKS)),
            dma((levels, CHUNKS)),
            dma((low, CHUNKS)),
            dma((low, CHUNKS)),
            dma((CHUNKS,)),
            dma((CHUNKS,)),
        ],
        compiler_params=pltpu.CompilerParams(collective_id=0, has_side_effects=True),
    )(random_block, diag_block, basis_out, basis_in, low_up, low_down, low_coupling,
      top_up, top_down, top_coupling)


def solution(mesh):
    rows = P("leaf", None)
    gens = P("leaf", None, None, None)
    return jax.shard_map(
        per_device, mesh=mesh,
        in_specs=(rows, rows, rows, rows, gens, gens, gens, P(), P(), P()),
        out_specs=rows, check_vma=False,
    )
```
